256 devices in a mesh: dp: 4 (over y), seq: 64 (over x, z, core).
Axes of the slice: x: 4, y: 4, z: 8, core: 2. Of those that a mesh axis runs over, the one named last changes fastest.
Arguments:
- tokens: bfloat16 [262144, 1152], P(('dp', 'seq')), parts along dimension 0, may hold values from -6 to 6
- norm_gain: float32 [1152], replicated, may hold values from 0.4 to 2.5
- norm_bias: float32 [1152], replicated, may hold values from -3 to 3
- qkv_weight: bfloat16 [1152, 1728], replicated, may hold values from -1.5 to 1.5, as said below
- out_weight: bfloat16 [576, 1152], replicated, may hold values from -0.25 to 0.25
- segment_ids: int32 [262144], P(('dp', 'seq')), parts along dimension 0, may hold values from 0 to 65535, as said below
- dest_map: int32 [262144], P(('dp', 'seq')), parts along dimension 0, may hold values from 0 to 65535, as said below
Outputs:
- language: bfloat16 [262144, 1152], P(('dp', 'seq')), parts along dimension 0
The draws below stay inside these ranges and needn't reach their ends.
There are 4 independent parts, one for each index of `dp`. The reference program is written for one: setup_inputs(seed, part) draws one part's arguments, and reference() takes and returns one part's arrays. A program takes and returns all parts, laid end to end along the dimension named above; an argument that names none is the same for every part. Nothing has to cross between parts.
Inputs may be any that keep to these rules, and one draw needn't show every extreme that they name: `segment_ids`: ids never fall along the tokens; an image's tokens lie within one run of 1024 tokens, and within a run each new image takes the next id. In some run all tokens form one image. `dest_map`: A permutation. The tokens of one run go to exactly 32 runs of the language layout (row // 1024), exactly 32 tokens to each. `qkv_weight`: the three groups of columns are the query, key and value projections.
All inputs are finite; a program needn't handle non-finite values.
Results may differ from the reference program's by a relative error of at most 0.0057.
Values may be sent and summed in bfloat16 or wider, within the bound.
No kernel may reach another device: no remote copies, remote signals or barrier semaphores. Data moves between devices by JAX's collectives and lax.ppermute only.
A program may use at most 128 MiB of HBM per device.

```python
import math
import jax
import jax.numpy as jnp
from jax import lax

D = 1152
HEADS = 8
HEAD_DIM = 72
BLOCK = 128
TOK_DEV = 1024
TOKENS = 65536
N_SEQ = 64


def draw_qkv_weight(key, part):
    width = HEADS * HEAD_DIM
    first, second, third = jax.random.split(jax.random.fold_in(key, 5), 3)
    queries = jax.random.normal(first, (D, width), jnp.float32) * D ** (-0.5)
    values = jax.random.normal(third, (D, width), jnp.float32) * D ** (-0.5)
    noise = jax.random.normal(second, (D, width), jnp.float32) * D ** (-0.5)
    keyed = noise
    joined = jnp.concatenate([queries, keyed, values], axis=1)
    return jnp.clip(joined, -1.5, 1.5).astype(jnp.bfloat16)


def draw_segment_ids(key, part):
    count_key, pick_key, order_key = jax.random.split(jax.random.fold_in(key, 11), 3)
    block_count = TOK_DEV // BLOCK
    cuts = jax.random.randint(count_key, (N_SEQ, 1), 0, 8 * block_count)
    picked = jax.random.randint(pick_key, (), 0, N_SEQ)
    cuts = jnp.where(jnp.arange(N_SEQ)[:, None] == picked, 0, cuts)
    ranks = jax.vmap(lambda single: jax.random.permutation(single, TOK_DEV))(jax.random.split(order_key, N_SEQ))
    starts = (ranks < cuts) & (jnp.arange(TOK_DEV)[None, :] > 0)
    local = jnp.cumsum(starts.astype(jnp.int32), axis=1)
    ids = jnp.arange(N_SEQ)[:, None] * TOK_DEV + local
    return ids.reshape(-1).astype(jnp.int32)


def draw_dest_map(key, part):
    groups = N_SEQ // 2
    capacity = TOK_DEV * 2 // N_SEQ
    offset_key, order_key = jax.random.split(jax.random.fold_in(key, 23))
    offsets = jax.random.permutation(offset_key, N_SEQ)[:groups]
    ranks = jax.vmap(lambda single: jax.random.permutation(single, TOK_DEV))(jax.random.split(order_key, N_SEQ))
    group = ranks // capacity
    within = ranks % capacity
    source = jnp.arange(N_SEQ)[:, None]
    target = (source + offsets[group]) % N_SEQ
    position = group * capacity + within
    return (target * TOK_DEV + position).reshape(-1).astype(jnp.int32)


def shard_levels(rng, extent, pieces, low, top_value):
    def one(axis_at, shards_of):
        heights = jax.random.uniform(jax.random.fold_in(jax.random.fold_in(rng, 6), axis_at), (shards_of,), jnp.float32, low / len(pieces), top_value / len(pieces))
        return jnp.repeat(jnp.exp(heights), extent[axis_at] // shards_of).reshape((-1,) + (1,) * (len(extent) - axis_at - 1))

    factor_of = one(*pieces[0])
    for cut in pieces[1:]:
        factor_of = factor_of * one(*cut)
    return factor_of


def normal_values(stream_key, dims, scale, most, cuts=(), kind=jnp.bfloat16):
    values = scale * jax.random.normal(stream_key, dims, jnp.float32)
    if cuts:
        values = values * shard_levels(stream_key, dims, cuts, -0.22, 0.18)
    return jnp.clip(values, -most, most).astype(kind)


def setup_inputs(seed: int = 0, part: int = 0) -> dict:
    streams_of = jax.random.split(jax.random.key(seed), 8)
    part_keys = jax.random.split(jax.random.fold_in(streams_of[7], part), 8)
    return {
        "tokens": normal_values(part_keys[0], (TOKENS, D), 1.0, 6.0, ((0, 64),)),
        "norm_gain": jnp.clip(jnp.exp(jax.random.uniform(streams_of[1], (D,), jnp.float32, math.log(0.4), math.log(2.5))), 0.4, 2.5),
        "norm_bias": normal_values(streams_of[2], (D,), 0.5, 3.0, (), jnp.float32),
        "qkv_weight": draw_qkv_weight(jax.random.fold_in(streams_of[7], 71), part),
        "out_weight": normal_values(streams_of[4], (HEADS * HEAD_DIM, D), (HEADS * HEAD_DIM) ** -0.5, 0.25),
        "segment_ids": draw_segment_ids(jax.random.fold_in(jax.random.fold_in(streams_of[7], part), 71), part),
        "dest_map": draw_dest_map(jax.random.fold_in(jax.random.fold_in(streams_of[7], part), 71), part),
    }


masked_fill = -1e+30

def normalize(row_block, norm_gain, norm_bias):
    values = row_block.astype(jnp.float32)
    center = values - lax.optimization_barrier(jnp.mean(values, axis=1, keepdims=True))
    spread = lax.optimization_barrier(jnp.mean(center * center, axis=1, keepdims=True))
    scaled = center * lax.rsqrt(spread + 1e-06) * norm_gain + norm_bias
    return scaled.astype(jnp.bfloat16)

def pair_partial(queries, key_block, value_block, query_ids, key_ids):
    scores = jnp.einsum('hdq,hdk->hqk', queries.astype(jnp.float32), key_block.astype(jnp.float32)) * HEAD_DIM ** (-0.5)
    allowed = (query_ids[:, None] == key_ids[None, :])[None]
    masked = jnp.where(allowed, scores, masked_fill)
    maxima = lax.optimization_barrier(jnp.max(masked, axis=2))
    weights = jnp.where(allowed, jnp.exp(masked - maxima[:, :, None]), 0.0)
    totals = lax.optimization_barrier(jnp.sum(weights, axis=2))
    rounded = weights.astype(jnp.bfloat16).astype(jnp.float32)
    summed = jnp.einsum('hqk,hdk->hdq', rounded, value_block.astype(jnp.float32))
    return (maxima, totals, summed)

def reference(tokens, norm_gain, norm_bias, qkv_weight, out_weight, segment_ids, dest_map):
    block_count = TOK_DEV // BLOCK
    pair_count = block_count * block_count
    pair_query = (jnp.arange(pair_count) // block_count).astype(jnp.int32)
    pair_keys = (jnp.arange(pair_count) % block_count).astype(jnp.int32)
    weight_heads = out_weight.reshape(HEADS, HEAD_DIM, D).astype(jnp.float32)

    def one_run(inputs):
        row_block, run_ids = inputs
        normed = normalize(row_block, norm_gain, norm_bias)
        projected = jnp.dot(normed, qkv_weight, preferred_element_type=jnp.float32).astype(jnp.bfloat16)
        blocks = projected.reshape(block_count, BLOCK, 3, HEADS, HEAD_DIM).transpose(0, 2, 3, 4, 1)
        id_blocks = run_ids.reshape(block_count, BLOCK)

        def one_pair(pair_index):
            q_block = pair_query[pair_index]
            k_block = pair_keys[pair_index]
            return pair_partial(blocks[q_block, 0], blocks[k_block, 1], blocks[k_block, 2], id_blocks[q_block], id_blocks[k_block])
        maxima, totals, summed = lax.map(one_pair, jnp.arange(pair_count, dtype=jnp.int32))
        maxima = maxima.reshape(block_count, block_count, HEADS, BLOCK)
        totals = totals.reshape(block_count, block_count, HEADS, BLOCK)
        summed = summed.reshape(block_count, block_count, HEADS, HEAD_DIM, BLOCK)
        highest = lax.optimization_barrier(jnp.max(maxima, axis=1))
        scales = jnp.exp(maxima - highest[:, None])
        denom = lax.optimization_barrier(jnp.sum(scales * totals, axis=1))
        numer = lax.optimization_barrier(jnp.sum(scales[:, :, :, None, :] * summed, axis=1))
        attended = (numer / denom[:, :, None, :]).astype(jnp.bfloat16)
        mixed = jnp.einsum('nhdb,hde->nbe', attended.astype(jnp.float32), weight_heads).reshape(TOK_DEV, D)
        return (row_block.astype(jnp.float32) + mixed).astype(jnp.bfloat16)
    vision = lax.map(one_run, (tokens.reshape(N_SEQ, TOK_DEV, D), segment_ids.reshape(N_SEQ, TOK_DEV)))
    vision = vision.reshape(TOKENS, D)
    return jnp.zeros_like(vision).at[dest_map].set(vision)
```

```python
import math

import jax
import jax.numpy as jnp
from jax import lax
from jax.experimental import pallas as pl
from jax.experimental.pallas import tpu as pltpu
from jax.sharding import PartitionSpec as P

HEADS = 8
HEAD_DIM = 72
WIDTH = HEADS * HEAD_DIM
RUN = 1024
N_SEQ = 64
GROUPS = 32
CAP = 32
D = 1152
LANES = 128
SHIFT = 64
PADDED = 640
ROWS = 256
KEYS = 256
PACK = 16
COLUMNS = D // LANES
PAYLOAD = CAP * COLUMNS
SLOT = PAYLOAD + 8
MASKED = -1e30
SCORE_SCALE = HEAD_DIM ** (-0.5) * math.log2(math.e)

f32 = jnp.float32
bf16 = jnp.bfloat16
NT = (((1,), (1,)), ((), ()))
TN = (((0,), (0,)), ((), ()))


def iota(shape, axis):
    return lax.broadcasted_iota(jnp.int32, shape, axis)


def window(low):
    a, b = low // LANES * LANES, -(-(low + HEAD_DIM) // LANES) * LANES
    lane = iota((1, b - a), 1) + a
    return a, b, (lane >= low) & (lane < low + HEAD_DIM)


def compact(used):
    flags = jnp.broadcast_to(used.astype(f32), (N_SEQ, LANES)).astype(bf16)
    lower = (iota((N_SEQ, N_SEQ), 1) < iota((N_SEQ, N_SEQ), 0)).astype(f32).astype(bf16)
    before = jnp.dot(lower, flags, preferred_element_type=f32).astype(jnp.int32)
    return (before == iota((N_SEQ, LANES), 1)) & used


def names_of(chosen):
    return jnp.sum(jnp.where(chosen, iota((N_SEQ, LANES), 0), 0), axis=0, keepdims=True)


def front_kernel(
    tok_hbm, gain_hbm, bias_hbm, w_hbm, ow_hbm, seg_hbm, dest_hbm, send_ref,
    tok_ref, w_ref, ow_ref, moved_ref, q_ref, key_ref, value_ref, seg_row_ref, seg_col_ref,
    mask_ref, score_ref, att_ref, gain_ref, bias_ref, seg_ref, dest_ref, ids_vec, ids_ref, sems,
):
    copies = [
        pltpu.make_async_copy(source, held, sems.at[n])
        for n, (source, held) in enumerate(
            (
                (dest_hbm, dest_ref),
                (seg_hbm, seg_ref),
                (tok_hbm, tok_ref),
                (gain_hbm, gain_ref),
                (bias_hbm, bias_ref),
                (w_hbm, w_ref),
                (ow_hbm, ow_ref),
            )
        )
    ]
    for copy in copies:
        copy.start()
    copies[0].wait()

    dest = dest_ref[...]
    target = dest // RUN
    place = dest % RUN
    slot = iota((N_SEQ, RUN), 0)
    hit = slot == target
    hits = hit.astype(f32).astype(bf16)
    upto = (iota((LANES, LANES), 0) <= iota((LANES, LANES), 1)).astype(f32).astype(bf16)
    before = jnp.zeros((N_SEQ, 1), f32)
    ranks = []
    for tile in range(RUN // LANES):
        running = jnp.dot(hits[:, tile * LANES : (tile + 1) * LANES], upto, preferred_element_type=f32)
        ranks.append(running + before)
        before = before + running[:, LANES - 1 :]
    used = before > 0
    rank = jnp.sum(jnp.where(hit, jnp.concatenate(ranks, axis=1), 0.0), axis=0, keepdims=True)
    rank = rank.astype(jnp.int32) - 1
    block = jnp.sum(jnp.where((slot < target) & used, 1.0, 0.0), axis=0, keepdims=True)
    order = block.astype(jnp.int32) * CAP + rank

    ids_vec[...] = names_of(compact(used))
    ids_copy = pltpu.make_async_copy(ids_vec, ids_ref, sems.at[7])
    ids_copy.start()

    at_rank = iota((LANES, RUN), 0) % CAP == rank

    def spread(row):
        chosen = jnp.where(at_rank, row.astype(f32), 0.0).astype(bf16)
        return lax.dot_general(hits, chosen, NT, preferred_element_type=f32)

    there = spread(jnp.ones_like(place)) > 0
    high = jnp.where(there, spread(place // CAP), RUN // CAP)
    low = spread(place % CAP)
    top_row = iota((8, LANES), 0) == 0
    send_ref[:, :PAYLOAD] = jnp.zeros((N_SEQ, PAYLOAD, LANES), bf16)
    for s in range(N_SEQ):
        send_ref[s, PAYLOAD:] = jnp.where(top_row, high[s : s + 1], low[s : s + 1]).astype(bf16)

    copies[1].wait()
    seg = seg_ref[...]
    digit = iota((8, RUN), 0)
    digits = jnp.where(digit == 0, seg % 256, jnp.where(digit == 1, seg // 256, 0)).astype(f32).astype(bf16)
    digits_wide = jnp.concatenate([digits, jnp.zeros((LANES - 8, RUN), bf16)], axis=0)

    att_ref[...] = jnp.zeros_like(att_ref)
    for copy in copies[2:6]:
        copy.wait()
    gain = gain_ref[...].reshape(1, D)
    shift = bias_ref[...].reshape(1, D)
    for step in range(RUN // ROWS):
        rows = slice(step * ROWS, (step + 1) * ROWS)
        move = (order == iota((ROWS, RUN), 0) + step * ROWS).astype(f32).astype(bf16)
        moved = jnp.dot(move, tok_ref[...], preferred_element_type=f32)
        columns = lax.dot_general(move, digits_wide, NT, preferred_element_type=f32)
        across = lax.dot_general(digits, move, NT, preferred_element_type=f32)
        seg_row_ref[:, rows] = jnp.broadcast_to(across[0:1] + 256.0 * across[1:2], (8, ROWS))
        column = columns[:, 0:1] + 256.0 * columns[:, 1:2]
        seg_col_ref[rows] = jnp.broadcast_to(column, (ROWS, LANES))
        moved_ref[rows] = moved.astype(bf16)
        center = moved - jnp.mean(moved, axis=1, keepdims=True)
        spread_of = jnp.mean(center * center, axis=1, keepdims=True)
        normed = (center * lax.rsqrt(spread_of + 1e-06) * gain + shift).astype(bf16)
        projected = lax.dot_general(normed, w_ref[...], NT, preferred_element_type=f32)
        q_ref[rows] = (pltpu.roll(projected[:, :PADDED], SHIFT, 1) * SCORE_SCALE).astype(bf16)
        key_ref[rows] = projected[:, WIDTH - SHIFT : WIDTH - SHIFT + PADDED].astype(bf16)
        values = projected[:, 2 * WIDTH :].astype(bf16)
        values = jnp.concatenate([values, jnp.ones((ROWS, PADDED - WIDTH), bf16)], axis=1)
        for head in range(HEADS):
            a, b, own = window(head * HEAD_DIM)
            value_ref[head, rows, : b - a] = jnp.where(own, values[:, a:b], 1)
    ids_copy.wait()
    copies[6].wait()

    def body(step, carry):
        row = pl.multiple_of(step * ROWS, ROWS)
        rows = pl.ds(row, ROWS)
        mask_ref[...] = jnp.where(seg_col_ref[rows, 0:1] == seg_row_ref[0:1, :], 0.0, MASKED)
        top = None
        for head in range(HEADS + 1):
            if head < HEADS:
                a, b, own = window(SHIFT + head * HEAD_DIM)
                query = jnp.where(own, q_ref[rows, a:b], 0)
            next_top = None
            summed = None
            for first in range(0, RUN, KEYS):
                keys = slice(first, first + KEYS)
                if head < HEADS:
                    scores = lax.dot_general(query, key_ref[keys, a:b], NT, preferred_element_type=f32)
                    scores = scores + mask_ref[:, keys]
                    score_ref[head % 2, :, keys] = scores
                    highest = scores[:, :LANES]
                    for tile in range(LANES, KEYS, LANES):
                        highest = jnp.maximum(highest, scores[:, tile : tile + LANES])
                    next_top = highest if next_top is None else jnp.maximum(next_top, highest)
                if head > 0:
                    low_, high_, _ = window((head - 1) * HEAD_DIM)
                    weights = jnp.exp2(score_ref[(head - 1) % 2, :, keys] - top).astype(bf16)
                    part = jnp.dot(
                        weights, value_ref[head - 1, keys, : high_ - low_], preferred_element_type=f32
                    )
                    summed = part if summed is None else summed + part
            if head > 0:
                start = (head - 1) * HEAD_DIM
                low_, high_, mine = window(start)
                spare = start - low_ - 1 if start > low_ else start + HEAD_DIM - low_
                mixed = (summed * (1.0 / summed[:, spare : spare + 1])).astype(bf16)
                att_ref[:, low_:high_] = jnp.where(mine, mixed, att_ref[:, low_:high_])
            if head < HEADS:
                top = jnp.max(next_top, axis=1, keepdims=True)
        mixed = jnp.dot(att_ref[:, :WIDTH], ow_ref[...], preferred_element_type=f32)
        vision = (moved_ref[rows].astype(f32) + mixed).astype(bf16)
        for block in range(ROWS // CAP):
            to = ids_ref[0, step * (ROWS // CAP) + block]
            for piece in range(CAP // PACK):
                at = block * CAP + piece * PACK
                for column in range(COLUMNS):
                    unit = (piece * COLUMNS + column) * PACK
                    send_ref[to, unit : unit + PACK] = vision[
                        at : at + PACK, column * LANES : (column + 1) * LANES
                    ]
        return carry

    lax.fori_loop(0, RUN // ROWS, body, 0)


def whole(memory=pltpu.VMEM):
    return pl.BlockSpec(memory_space=memory)


def front(tokens, norm_gain, norm_bias, qkv_weight, out_weight, segment_ids, dest_map):
    return pl.pallas_call(
        front_kernel,
        out_shape=jax.ShapeDtypeStruct((N_SEQ, SLOT, LANES), bf16),
        in_specs=[whole(pltpu.HBM)] * 7,
        out_specs=whole(),
        scratch_shapes=[
            pltpu.VMEM((RUN, D), bf16),
            pltpu.VMEM((3 * WIDTH, D), bf16),
            pltpu.VMEM((WIDTH, D), bf16),
            pltpu.VMEM((RUN, D), bf16),
            pltpu.VMEM((RUN, PADDED), bf16),
            pltpu.VMEM((RUN, PADDED), bf16),
            pltpu.VMEM((HEADS, RUN, 2 * LANES), bf16),
            pltpu.VMEM((8, RUN), f32),
            pltpu.VMEM((RUN, LANES), f32),
            pltpu.VMEM((ROWS, RUN), f32),
            pltpu.VMEM((2, ROWS, RUN), f32),
            pltpu.VMEM((ROWS, PADDED), bf16),
            pltpu.VMEM((D,), f32),
            pltpu.VMEM((D,), f32),
            pltpu.VMEM((1, RUN), jnp.int32),
            pltpu.VMEM((1, RUN), jnp.int32),
            pltpu.VMEM((1, LANES), jnp.int32),
            pltpu.SMEM((1, LANES), jnp.int32),
            pltpu.SemaphoreType.DMA((8,)),
        ],
        compiler_params=pltpu.CompilerParams(vmem_limit_bytes=67000000),
        name="front",
    )(
        tokens,
        norm_gain,
        norm_bias,
        qkv_weight.T,
        out_weight,
        segment_ids.reshape(1, RUN),
        dest_map.reshape(1, RUN),
    )


def unpack_kernel(got_ref, out_ref, rows_ref, ids_vec, place_ref, ids_ref, sem):
    step = pl.program_id(0)

    @pl.when(step == 0)
    def _():
        notes = got_ref[:, PAYLOAD:].astype(f32)
        first = iota(notes.shape, 1)
        high = jnp.sum(jnp.where(first == 0, notes, 0.0), axis=1)
        low = jnp.sum(jnp.where(first == 1, notes, 0.0), axis=1)
        chosen = compact(high[:, :1] < RUN // CAP)
        ids_vec[...] = names_of(chosen)
        copy = pltpu.make_async_copy(ids_vec, ids_ref, sem)
        copy.start()
        pick = chosen.astype(f32).astype(bf16)
        highs = lax.dot_general(pick, high.astype(bf16), TN, preferred_element_type=f32)
        lows = lax.dot_general(pick, low.astype(bf16), TN, preferred_element_type=f32)
        mine = iota((LANES, LANES), 1) // CAP == iota((LANES, LANES), 0) % (LANES // CAP)
        fold = (iota((8, LANES), 1) // (LANES // CAP) == iota((8, LANES), 0)).astype(f32).astype(bf16)

        def folded(values):
            return jnp.dot(fold, jnp.where(mine, values, 0.0).astype(bf16), preferred_element_type=f32)

        place_ref[...] = (folded(highs) * CAP + folded(lows)).astype(jnp.int32)
        copy.wait()
        for block in range(GROUPS):
            source = ids_ref[0, block]
            for piece in range(CAP // PACK):
                at = block * CAP + piece * PACK
                for column in range(COLUMNS):
                    unit = (piece * COLUMNS + column) * PACK
                    rows_ref[at : at + PACK, column * LANES : (column + 1) * LANES] = got_ref[
                        source, unit : unit + PACK
                    ]

    row = iota((ROWS, LANES), 0) + step * ROWS
    put = jnp.concatenate(
        [(place_ref[tile : tile + 1] == row).astype(f32).astype(bf16) for tile in range(RUN // LANES)], axis=1
    )
    out_ref[...] = jnp.dot(put, rows_ref[...], preferred_element_type=f32).astype(bf16)


def unpack(got):
    return pl.pallas_call(
        unpack_kernel,
        grid=(RUN // ROWS,),
        out_shape=jax.ShapeDtypeStruct((RUN, D), bf16),
        in_specs=[whole()],
        out_specs=pl.BlockSpec((ROWS, D), lambda i: (i, 0)),
        scratch_shapes=[
            pltpu.VMEM((RUN, D), bf16),
            pltpu.VMEM((1, LANES), jnp.int32),
            pltpu.VMEM((8, LANES), jnp.int32),
            pltpu.SMEM((1, LANES), jnp.int32),
            pltpu.SemaphoreType.DMA(()),
        ],
        compiler_params=pltpu.CompilerParams(vmem_limit_bytes=30 * 2**20),
        name="unpack",
    )(got)


def local(tokens, norm_gain, norm_bias, qkv_weight, out_weight, segment_ids, dest_map):
    sent = front(tokens, norm_gain, norm_bias, qkv_weight, out_weight, segment_ids, dest_map)
    got = lax.all_to_all(sent, "seq", split_axis=0, concat_axis=0, tiled=True)
    return unpack(got)


def solution(mesh):
    placed = (P(("dp", "seq"), None), P(), P(), P(), P(), P(("dp", "seq")), P(("dp", "seq")))
    return jax.shard_map(
        local, mesh=mesh, in_specs=placed, out_specs=P(("dp", "seq"), None), check_vma=False
    )
```

```python
import math

import jax
import jax.numpy as jnp
from jax import lax
from jax.experimental import pallas as pl
from jax.experimental.pallas import tpu as pltpu
from jax.sharding import PartitionSpec as P

HEADS = 8
HEAD_DIM = 72
WIDTH = HEADS * HEAD_DIM
RUN = 1024
N_SEQ = 64
GROUPS = 32
CAP = 32
D = 1152
LANES = 128
SHIFT = 64
PADDED = 640
ROWS = 256
QUERIES = 512
KEYS = 512
PACK = 16
COLUMNS = D // LANES
PAYLOAD = CAP * COLUMNS
SLOT = PAYLOAD + 8
MASKED = -1e30
SCORE_SCALE = HEAD_DIM ** (-0.5) * math.log2(math.e)

f32 = jnp.float32
bf16 = jnp.bfloat16
NT = (((1,), (1,)), ((), ()))
TN = (((0,), (0,)), ((), ()))


def iota(shape, axis):
    return lax.broadcasted_iota(jnp.int32, shape, axis)


def window(low):
    a, b = low // LANES * LANES, -(-(low + HEAD_DIM) // LANES) * LANES
    lane = iota((1, b - a), 1) + a
    return a, b, (lane >= low) & (lane < low + HEAD_DIM)


def compact(used):
    flags = jnp.broadcast_to(used.astype(f32), (N_SEQ, LANES)).astype(bf16)
    lower = (iota((N_SEQ, N_SEQ), 1) < iota((N_SEQ, N_SEQ), 0)).astype(f32).astype(bf16)
    before = jnp.dot(lower, flags, preferred_element_type=f32).astype(jnp.int32)
    return (before == iota((N_SEQ, LANES), 1)) & used


def names_of(chosen):
    return jnp.sum(jnp.where(chosen, iota((N_SEQ, LANES), 0), 0), axis=0, keepdims=True)


def front_kernel(
    tok_hbm, gain_hbm, bias_hbm, w_hbm, ow_hbm, seg_hbm, dest_hbm, send_ref,
    tok_ref, w_ref, ow_ref, moved_ref, q_ref, key_ref, value_ref, seg_row_ref, seg_col_ref,
    mask_ref, score_ref, att_ref, gain_ref, bias_ref, seg_ref, dest_ref, ids_vec, ids_ref, sems,
):
    copies = [
        pltpu.make_async_copy(source, held, sems.at[n])
        for n, (source, held) in enumerate(
            (
                (dest_hbm, dest_ref),
                (seg_hbm, seg_ref),
                (tok_hbm, tok_ref.at[:, :D]),
                (gain_hbm, gain_ref),
                (bias_hbm, bias_ref),
                (w_hbm, w_ref),
                (ow_hbm, ow_ref),
            )
        )
    ]
    for copy in copies[:3]:
        copy.start()
    copies[0].wait()

    dest = dest_ref[...]
    target = dest // RUN
    place = dest % RUN
    slot = iota((N_SEQ, RUN), 0)
    hit = slot == target
    hits = hit.astype(f32).astype(bf16)
    upto = (iota((LANES, LANES), 0) <= iota((LANES, LANES), 1)).astype(f32).astype(bf16)
    before = jnp.zeros((N_SEQ, 1), f32)
    ranks = []
    for tile in range(RUN // LANES):
        running = jnp.dot(hits[:, tile * LANES : (tile + 1) * LANES], upto, preferred_element_type=f32)
        ranks.append(running + before)
        before = before + running[:, LANES - 1 :]
    used = before > 0
    rank = jnp.sum(jnp.where(hit, jnp.concatenate(ranks, axis=1), 0.0), axis=0, keepdims=True)
    rank = rank.astype(jnp.int32) - 1
    block = jnp.sum(jnp.where((slot < target) & used, 1.0, 0.0), axis=0, keepdims=True)
    order = block.astype(jnp.int32) * CAP + rank

    ids_vec[...] = names_of(compact(used))
    ids_copy = pltpu.make_async_copy(ids_vec, ids_ref, sems.at[7])
    ids_copy.start()

    at_rank = iota((LANES, RUN), 0) % CAP == rank

    def spread(row):
        chosen = jnp.where(at_rank, row.astype(f32), 0.0).astype(bf16)
        return lax.dot_general(hits, chosen, NT, preferred_element_type=f32)

    there = spread(jnp.ones_like(place)) > 0
    high = jnp.where(there, spread(place // CAP), RUN // CAP)
    low = spread(place % CAP)
    top_row = iota((8, LANES), 0) == 0
    for s in range(N_SEQ):
        send_ref[s, PAYLOAD:] = jnp.where(top_row, high[s : s + 1], low[s : s + 1]).astype(bf16)

    copies[1].wait()
    seg = seg_ref[...]
    digit = iota((LANES, RUN), 0)
    digits = jnp.where(digit == 0, seg % 256, jnp.where(digit == 1, seg // 256, 0)).astype(f32)
    for tile in range(RUN // LANES):
        part = slice(tile * LANES, (tile + 1) * LANES)
        tok_ref[part, D:] = jnp.transpose(digits[:, part]).astype(bf16)
    digits = digits[:8].astype(bf16)

    att_ref[...] = jnp.zeros_like(att_ref)
    copies[2].wait()
    for copy in copies[3:]:
        copy.start()
    for step in range(RUN // ROWS):
        rows = slice(step * ROWS, (step + 1) * ROWS)
        move = (order == iota((ROWS, RUN), 0) + step * ROWS).astype(f32).astype(bf16)
        moved = jnp.dot(move, tok_ref[...], preferred_element_type=f32)
        across = lax.dot_general(digits, move, NT, preferred_element_type=f32)
        seg_row_ref[:, rows] = jnp.broadcast_to(across[0:1] + 256.0 * across[1:2], (8, ROWS))
        column = moved[:, D : D + 1] + 256.0 * moved[:, D + 1 : D + 2]
        seg_col_ref[rows] = jnp.broadcast_to(column, (ROWS, LANES))
        moved_ref[rows] = moved[:, :D].astype(bf16)
    for copy in copies[3:6]:
        copy.wait()
    gain = gain_ref[...].reshape(1, D)
    shift = bias_ref[...].reshape(1, D)
    for step in range(RUN // ROWS):
        rows = slice(step * ROWS, (step + 1) * ROWS)
        moved = moved_ref[rows].astype(f32)
        center = moved - jnp.mean(moved, axis=1, keepdims=True)
        spread_of = jnp.mean(center * center, axis=1, keepdims=True)
        normed = (center * lax.rsqrt(spread_of + 1e-06) * gain + shift).astype(bf16)
        projected = lax.dot_general(normed, w_ref[...], NT, preferred_element_type=f32)
        q_ref[rows] = (pltpu.roll(projected[:, :PADDED], SHIFT, 1) * SCORE_SCALE).astype(bf16)
        key_ref[rows] = projected[:, WIDTH - SHIFT : WIDTH - SHIFT + PADDED].astype(bf16)
        values = projected[:, 2 * WIDTH :].astype(bf16)
        values = jnp.concatenate([values, jnp.ones((ROWS, PADDED - WIDTH), bf16)], axis=1)
        for head in range(HEADS):
            a, b, own = window(head * HEAD_DIM)
            value_ref[head, rows, : b - a] = jnp.where(own, values[:, a:b], 1)
    ids_copy.wait()
    copies[6].wait()

    def body(step, carry):
        row = pl.multiple_of(step * QUERIES, QUERIES)
        rows = pl.ds(row, QUERIES)
        mask_ref[...] = jnp.where(seg_col_ref[rows, 0:1] == seg_row_ref[0:1, :], 0.0, MASKED)
        top = None
        for head in range(HEADS + 1):
            if head < HEADS:
                a, b, own = window(SHIFT + head * HEAD_DIM)
                query = jnp.where(own, q_ref[rows, a:b], 0)
            next_top = None
            summed = None
            for first in range(0, RUN, KEYS):
                keys = slice(first, first + KEYS)
                if head < HEADS:
                    scores = lax.dot_general(query, key_ref[keys, a:b], NT, preferred_element_type=f32)
                    scores = scores + mask_ref[:, keys]
                    score_ref[head % 2, :, keys] = scores
                    highest = scores[:, :LANES]
                    for tile in range(LANES, KEYS, LANES):
                        highest = jnp.maximum(highest, scores[:, tile : tile + LANES])
                    next_top = highest if next_top is None else jnp.maximum(next_top, highest)
                if head > 0:
                    low_, high_, _ = window((head - 1) * HEAD_DIM)
                    weights = jnp.exp2(score_ref[(head - 1) % 2, :, keys] - top).astype(bf16)
                    part = jnp.dot(
                        weights, value_ref[head - 1, keys, : high_ - low_], preferred_element_type=f32
                    )
                    summed = part if summed is None else summed + part
            if head > 0:
                start = (head - 1) * HEAD_DIM
                low_, high_, mine = window(start)
                spare = start - low_ - 1 if start > low_ else start + HEAD_DIM - low_
                mixed = (summed * (1.0 / summed[:, spare : spare + 1])).astype(bf16)
                att_ref[:, low_:high_] = jnp.where(mine, mixed, att_ref[:, low_:high_])
            if head < HEADS:
                top = jnp.max(next_top, axis=1, keepdims=True)
        mixed = jnp.dot(att_ref[:, :WIDTH], ow_ref[...], preferred_element_type=f32)
        vision = (moved_ref[rows].astype(f32) + mixed).astype(bf16)
        for block in range(QUERIES // CAP):
            to = ids_ref[0, step * (QUERIES // CAP) + block]
            for piece in range(CAP // PACK):
                at = block * CAP + piece * PACK
                for column in range(COLUMNS):
                    unit = (piece * COLUMNS + column) * PACK
                    send_ref[to, unit : unit + PACK] = vision[
                        at : at + PACK, column * LANES : (column + 1) * LANES
                    ]
        return carry

    lax.fori_loop(0, RUN // QUERIES, body, 0)


def whole(memory=pltpu.VMEM):
    return pl.BlockSpec(memory_space=memory)


def front(tokens, norm_gain, norm_bias, qkv_weight, out_weight, segment_ids, dest_map):
    return pl.pallas_call(
        front_kernel,
        out_shape=pltpu.VMEM((N_SEQ, SLOT, LANES), bf16),
        in_specs=[whole(pltpu.HBM)] * 7,
        out_specs=whole(),
        scratch_shapes=[
            pltpu.VMEM((RUN, D + LANES), bf16),
            pltpu.VMEM((3 * WIDTH, D), bf16),
            pltpu.VMEM((WIDTH, D), bf16),
            pltpu.VMEM((RUN, D), bf16),
            pltpu.VMEM((RUN, PADDED), bf16),
            pltpu.VMEM((RUN, PADDED), bf16),
            pltpu.VMEM((HEADS, RUN, 2 * LANES), bf16),
            pltpu.VMEM((8, RUN), f32),
            pltpu.VMEM((RUN, LANES), f32),
            pltpu.VMEM((QUERIES, RUN), f32),
            pltpu.VMEM((2, QUERIES, RUN), f32),
            pltpu.VMEM((QUERIES, PADDED), bf16),
            pltpu.VMEM((D,), f32),
            pltpu.VMEM((D,), f32),
            pltpu.VMEM((1, RUN), jnp.int32),
            pltpu.VMEM((1, RUN), jnp.int32),
            pltpu.VMEM((1, LANES), jnp.int32),
            pltpu.SMEM((1, LANES), jnp.int32),
            pltpu.SemaphoreType.DMA((8,)),
        ],
        compiler_params=pltpu.CompilerParams(vmem_limit_bytes=46 * 2**20),
        name="front",
    )(
        *(
            pltpu.with_memory_space_constraint(x, pltpu.HBM)
            for x in (
                tokens,
                norm_gain,
                norm_bias,
                qkv_weight.T,
                out_weight,
                segment_ids.reshape(1, RUN),
                dest_map.reshape(1, RUN),
            )
        )
    )


def unpack_kernel(got_ref, out_hbm, rows_ref, out_ref, ids_vec, ids_ref, sems):
    notes = got_ref[:, PAYLOAD:].astype(f32)
    first = iota(notes.shape, 1)
    high = jnp.sum(jnp.where(first == 0, notes, 0.0), axis=1)
    low = jnp.sum(jnp.where(first == 1, notes, 0.0), axis=1)
    chosen = compact(high[:, :1] < RUN // CAP)
    ids_vec[...] = names_of(chosen)
    ids_copy = pltpu.make_async_copy(ids_vec, ids_ref, sems.at[0])
    ids_copy.start()
    pick = chosen.astype(f32).astype(bf16)
    highs = lax.dot_general(pick, high.astype(bf16), TN, preferred_element_type=f32)
    lows = lax.dot_general(pick, low.astype(bf16), TN, preferred_element_type=f32)
    mine = iota((LANES, LANES), 1) // CAP == iota((LANES, LANES), 0) % (LANES // CAP)
    fold = (iota((8, LANES), 1) // (LANES // CAP) == iota((8, LANES), 0)).astype(f32).astype(bf16)

    def folded(values):
        return jnp.dot(fold, jnp.where(mine, values, 0.0).astype(bf16), preferred_element_type=f32)

    places = (folded(highs) * CAP + folded(lows)).astype(jnp.int32)
    ids_copy.wait()
    for block in range(GROUPS):
        source = ids_ref[0, block]
        for piece in range(CAP // PACK):
            at = block * CAP + piece * PACK
            for column in range(COLUMNS):
                unit = (piece * COLUMNS + column) * PACK
                rows_ref[at : at + PACK, column * LANES : (column + 1) * LANES] = got_ref[
                    source, unit : unit + PACK
                ]
    copies = []
    for step in range(RUN // ROWS):
        row = iota((ROWS, LANES), 0) + step * ROWS
        put = jnp.concatenate(
            [(places[tile : tile + 1] == row).astype(f32).astype(bf16) for tile in range(RUN // LANES)], axis=1
        )
        part = pl.ds(step * ROWS, ROWS)
        out_ref[part] = jnp.dot(put, rows_ref[...], preferred_element_type=f32).astype(bf16)
        copies.append(pltpu.make_async_copy(out_ref.at[part], out_hbm.at[part], sems.at[step + 1]))
        copies[-1].start()
    for copy in copies:
        copy.wait()


def unpack(got):
    return pl.pallas_call(
        unpack_kernel,
        out_shape=jax.ShapeDtypeStruct((RUN, D), bf16),
        in_specs=[whole()],
        out_specs=whole(pl.ANY),
        scratch_shapes=[
            pltpu.VMEM((RUN, D), bf16),
            pltpu.VMEM((RUN, D), bf16),
            pltpu.VMEM((1, LANES), jnp.int32),
            pltpu.SMEM((1, LANES), jnp.int32),
            pltpu.SemaphoreType.DMA((1 + RUN // ROWS,)),
        ],
        compiler_params=pltpu.CompilerParams(vmem_limit_bytes=40 * 2**20),
        name="unpack",
    )(got)


def local(tokens, norm_gain, norm_bias, qkv_weight, out_weight, segment_ids, dest_map):
    sent = front(tokens, norm_gain, norm_bias, qkv_weight, out_weight, segment_ids, dest_map)
    got = lax.all_to_all(sent, "seq", split_axis=0, concat_axis=0, tiled=True)
    return unpack(got)


def solution(mesh):
    placed = (P(("dp", "seq"), None), P(), P(), P(), P(), P(("dp", "seq")), P(("dp", "seq")))
    return jax.shard_map(
        local, mesh=mesh, in_specs=placed, out_specs=P(("dp", "seq"), None), check_vma=False
    )
```

```python
import math

import jax
import jax.numpy as jnp
from jax import lax
from jax.experimental import pallas as pl
from jax.experimental.pallas import tpu as pltpu
from jax.sharding import PartitionSpec as P

HEADS = 8
HEAD_DIM = 72
WIDTH = HEADS * HEAD_DIM
RUN = 1024
N_SEQ = 64
GROUPS = 32
CAP = 32
D = 1152
LANES = 128
SHIFT = 64
PADDED = 640
ROWS = 256
QUERIES = 256
KEYS = 512
TAKEN = (256, 256, 256, 128, 128)
PACK = 16
COLUMNS = D // LANES
PAYLOAD = CAP * COLUMNS
SLOT = PAYLOAD + 8
MASKED = -1e30
SCORE_SCALE = HEAD_DIM ** (-0.5) * math.log2(math.e)

f32 = jnp.float32
bf16 = jnp.bfloat16
NT = (((1,), (1,)), ((), ()))
TN = (((0,), (0,)), ((), ()))


def iota(shape, axis):
    return lax.broadcasted_iota(jnp.int32, shape, axis)


def window(low):
    a, b = low // LANES * LANES, -(-(low + HEAD_DIM) // LANES) * LANES
    lane = iota((1, b - a), 1) + a
    return a, b, (lane >= low) & (lane < low + HEAD_DIM)


def compact(used):
    flags = jnp.broadcast_to(used.astype(f32), (N_SEQ, LANES)).astype(bf16)
    lower = (iota((N_SEQ, N_SEQ), 1) < iota((N_SEQ, N_SEQ), 0)).astype(f32).astype(bf16)
    before = jnp.dot(lower, flags, preferred_element_type=f32).astype(jnp.int32)
    return (before == iota((N_SEQ, LANES), 1)) & used


def names_of(chosen):
    return jnp.sum(jnp.where(chosen, iota((N_SEQ, LANES), 0), 0), axis=0, keepdims=True)


def front_kernel(
    tok_hbm, gain_hbm, bias_hbm, w_hbm, ow_hbm, seg_hbm, dest_hbm, send_ref,
    tok_ref, w_ref, ow_ref, moved_ref, q_ref, key_ref, value_ref, seg_row_ref, seg_col_ref,
    mask_ref, score_ref, att_ref, gain_ref, bias_ref, seg_ref, dest_ref, ids_vec, ids_ref, sems,
):
    copies = [
        pltpu.make_async_copy(source, held, sems.at[n])
        for n, (source, held) in enumerate(
            (
                (dest_hbm, dest_ref),
                (seg_hbm, seg_ref),
                (tok_hbm, tok_ref.at[:, :D]),
                (gain_hbm, gain_ref),
                (bias_hbm, bias_ref),
                (w_hbm, w_ref),
                (ow_hbm, ow_ref),
            )
        )
    ]
    for copy in copies[:3]:
        copy.start()
    copies[0].wait()

    dest = dest_ref[...]
    target = dest // RUN
    place = dest % RUN
    slot = iota((N_SEQ, RUN), 0)
    hit = slot == target
    hits = hit.astype(f32).astype(bf16)
    upto = (iota((LANES, LANES), 0) <= iota((LANES, LANES), 1)).astype(f32).astype(bf16)
    before = jnp.zeros((N_SEQ, 1), f32)
    ranks = []
    for tile in range(RUN // LANES):
        running = jnp.dot(hits[:, tile * LANES : (tile + 1) * LANES], upto, preferred_element_type=f32)
        ranks.append(running + before)
        before = before + running[:, LANES - 1 :]
    used = before > 0
    rank = jnp.sum(jnp.where(hit, jnp.concatenate(ranks, axis=1), 0.0), axis=0, keepdims=True)
    rank = rank.astype(jnp.int32) - 1
    block = jnp.sum(jnp.where((slot < target) & used, 1.0, 0.0), axis=0, keepdims=True)
    order = block.astype(jnp.int32) * CAP + rank

    ids_vec[...] = names_of(compact(used))
    ids_copy = pltpu.make_async_copy(ids_vec, ids_ref, sems.at[7])
    ids_copy.start()

    at_rank = iota((LANES, RUN), 0) % CAP == rank

    def spread(row):
        chosen = jnp.where(at_rank, row.astype(f32), 0.0).astype(bf16)
        return lax.dot_general(hits, chosen, NT, preferred_element_type=f32)

    there = spread(jnp.ones_like(place)) > 0
    high = jnp.where(there, spread(place // CAP), RUN // CAP)
    low = spread(place % CAP)
    top_row = iota((8, LANES), 0) == 0
    for s in range(N_SEQ):
        send_ref[s, PAYLOAD:] = jnp.where(top_row, high[s : s + 1], low[s : s + 1]).astype(bf16)

    copies[1].wait()
    seg = seg_ref[...]
    digit = iota((LANES, RUN), 0)
    digits = jnp.where(digit == 0, seg % 256, jnp.where(digit == 1, seg // 256, 0)).astype(f32)
    for tile in range(RUN // LANES):
        part = slice(tile * LANES, (tile + 1) * LANES)
        tok_ref[part, D:] = jnp.transpose(digits[:, part]).astype(bf16)
    digits = digits[:8].astype(bf16)

    att_ref[...] = jnp.zeros_like(att_ref)
    copies[2].wait()
    for copy in copies[3:]:
        copy.start()
    for step in range(RUN // ROWS):
        rows = slice(step * ROWS, (step + 1) * ROWS)
        move = (order == iota((ROWS, RUN), 0) + step * ROWS).astype(f32).astype(bf16)
        moved = jnp.dot(move, tok_ref[...], preferred_element_type=f32)
        across = lax.dot_general(digits, move, NT, preferred_element_type=f32)
        seg_row_ref[:, rows] = jnp.broadcast_to(across[0:1] + 256.0 * across[1:2], (8, ROWS))
        column = moved[:, D : D + 1] + 256.0 * moved[:, D + 1 : D + 2]
        seg_col_ref[rows] = jnp.broadcast_to(column, (ROWS, LANES))
        moved_ref[rows] = moved[:, :D].astype(bf16)
    for copy in copies[3:6]:
        copy.wait()
    gain = gain_ref[...].reshape(1, D)
    shift = bias_ref[...].reshape(1, D)
    for step in range(RUN // ROWS):
        rows = slice(step * ROWS, (step + 1) * ROWS)
        moved = moved_ref[rows].astype(f32)
        center = moved - jnp.mean(moved, axis=1, keepdims=True)
        spread_of = jnp.mean(center * center, axis=1, keepdims=True)
        normed = (center * lax.rsqrt(spread_of + 1e-06) * gain + shift).astype(bf16)
        projected = lax.dot_general(normed, w_ref[...], NT, preferred_element_type=f32)
        q_ref[rows] = (pltpu.roll(projected[:, :PADDED], SHIFT, 1) * SCORE_SCALE).astype(bf16)
        key_ref[rows] = projected[:, WIDTH - SHIFT : WIDTH - SHIFT + PADDED].astype(bf16)
        values = projected[:, 2 * WIDTH :].astype(bf16)
        values = jnp.concatenate([values, jnp.ones((ROWS, PADDED - WIDTH), bf16)], axis=1)
        for head in range(HEADS):
            a, b, own = window(head * HEAD_DIM)
            value_ref[head, rows, : b - a] = jnp.where(own, values[:, a:b], 1)
    ids_copy.wait()
    copies[6].wait()

    units = [(part, head) for part in range(RUN // QUERIES) for head in range(HEADS)]

    def project(part, first, last):
        rows = slice(part * QUERIES, (part + 1) * QUERIES)
        mixed = jnp.dot(att_ref[part % 2, :, :WIDTH], ow_ref[:, first:last], preferred_element_type=f32)
        vision = (moved_ref[rows, first:last].astype(f32) + mixed).astype(bf16)
        for block in range(QUERIES // CAP):
            to = ids_ref[0, part * (QUERIES // CAP) + block]
            for piece in range(CAP // PACK):
                at = block * CAP + piece * PACK
                for column in range(first, last, LANES):
                    unit = (piece * COLUMNS + column // LANES) * PACK
                    send_ref[to, unit : unit + PACK] = vision[at : at + PACK, column - first : column - first + LANES]

    top = None
    for u in range(len(units) + 1):
        part, head = units[u] if u < len(units) else (None, None)
        done_part, done_head = units[u - 1] if u else (None, None)
        if head is not None:
            rows = slice(part * QUERIES, (part + 1) * QUERIES)
            if head == 0:
                same = seg_col_ref[rows, 0:1] == seg_row_ref[0:1, :]
                mask_ref[part % 2] = jnp.where(same, 0.0, MASKED)
            a, b, own = window(SHIFT + head * HEAD_DIM)
            query = jnp.where(own, q_ref[rows, a:b], 0)
        next_top = None
        summed = None
        for first in range(0, RUN, KEYS):
            keys = slice(first, first + KEYS)
            if head is not None:
                scores = lax.dot_general(query, key_ref[keys, a:b], NT, preferred_element_type=f32)
                scores = scores + mask_ref[part % 2, :, keys]
                score_ref[u % 2, :, keys] = scores
                highest = scores[:, :LANES]
                for tile in range(LANES, KEYS, LANES):
                    highest = jnp.maximum(highest, scores[:, tile : tile + LANES])
                next_top = highest if next_top is None else jnp.maximum(next_top, highest)
            if u:
                low_, high_, mine = window(done_head * HEAD_DIM)
                weights = jnp.exp2(score_ref[(u - 1) % 2, :, keys] - top).astype(bf16)
                piece = jnp.dot(
                    weights, value_ref[done_head, keys, : high_ - low_], preferred_element_type=f32
                )
                summed = piece if summed is None else summed + piece
        if u:
            start = done_head * HEAD_DIM
            spare = start - low_ - 1 if start > low_ else start + HEAD_DIM - low_
            mixed = (summed * (1.0 / summed[:, spare : spare + 1])).astype(bf16)
            held = att_ref.at[done_part % 2]
            held[:, low_:high_] = jnp.where(mine, mixed, held[:, low_:high_])
        if head is not None:
            top = jnp.max(next_top, axis=1, keepdims=True)
            if part and 1 <= head <= 5:
                project(part - 1, (head - 1) * ROWS, min(head * ROWS, D))
    project(RUN // QUERIES - 1, 0, D)


def whole(memory=pltpu.VMEM):
    return pl.BlockSpec(memory_space=memory)


def front(tokens, norm_gain, norm_bias, qkv_weight, out_weight, segment_ids, dest_map):
    return pl.pallas_call(
        front_kernel,
        out_shape=pltpu.VMEM((N_SEQ, SLOT, LANES), bf16),
        in_specs=[whole(pltpu.HBM)] * 7,
        out_specs=whole(),
        scratch_shapes=[
            pltpu.VMEM((RUN, D + LANES), bf16),
            pltpu.VMEM((3 * WIDTH, D), bf16),
            pltpu.VMEM((WIDTH, D), bf16),
            pltpu.VMEM((RUN, D), bf16),
            pltpu.VMEM((RUN, PADDED), bf16),
            pltpu.VMEM((RUN, PADDED), bf16),
            pltpu.VMEM((HEADS, RUN, 2 * LANES), bf16),
            pltpu.VMEM((8, RUN), f32),
            pltpu.VMEM((RUN, LANES), f32),
            pltpu.VMEM((2, QUERIES, RUN), f32),
            pltpu.VMEM((2, QUERIES, RUN), f32),
            pltpu.VMEM((2, QUERIES, PADDED), bf16),
            pltpu.VMEM((D,), f32),
            pltpu.VMEM((D,), f32),
            pltpu.VMEM((1, RUN), jnp.int32),
            pltpu.VMEM((1, RUN), jnp.int32),
            pltpu.VMEM((1, LANES), jnp.int32),
            pltpu.SMEM((1, LANES), jnp.int32),
            pltpu.SemaphoreType.DMA((8,)),
        ],
        compiler_params=pltpu.CompilerParams(vmem_limit_bytes=46 * 2**20),
        name="front",
    )(
        *(
            pltpu.with_memory_space_constraint(x, pltpu.HBM)
            for x in (
                tokens,
                norm_gain,
                norm_bias,
                qkv_weight.T,
                out_weight,
                segment_ids.reshape(1, RUN),
                dest_map.reshape(1, RUN),
            )
        )
    )


def unpack_kernel(got_ref, out_hbm, rows_ref, out_ref, ids_vec, ids_ref, sems):
    notes = got_ref[:, PAYLOAD:].astype(f32)
    first = iota(notes.shape, 1)
    high = jnp.sum(jnp.where(first == 0, notes, 0.0), axis=1)
    low = jnp.sum(jnp.where(first == 1, notes, 0.0), axis=1)
    chosen = compact(high[:, :1] < RUN // CAP)
    ids_vec[...] = names_of(chosen)
    ids_copy = pltpu.make_async_copy(ids_vec, ids_ref, sems.at[0])
    ids_copy.start()
    pick = chosen.astype(f32).astype(bf16)
    highs = lax.dot_general(pick, high.astype(bf16), TN, preferred_element_type=f32)
    lows = lax.dot_general(pick, low.astype(bf16), TN, preferred_element_type=f32)
    mine = iota((LANES, LANES), 1) // CAP == iota((LANES, LANES), 0) % (LANES // CAP)
    fold = (iota((8, LANES), 1) // (LANES // CAP) == iota((8, LANES), 0)).astype(f32).astype(bf16)

    def folded(values):
        return jnp.dot(fold, jnp.where(mine, values, 0.0).astype(bf16), preferred_element_type=f32)

    places = (folded(highs) * CAP + folded(lows)).astype(jnp.int32)
    ids_copy.wait()
    for block in range(GROUPS):
        source = ids_ref[0, block]
        for piece in range(CAP // PACK):
            at = block * CAP + piece * PACK
            for column in range(COLUMNS):
                unit = (piece * COLUMNS + column) * PACK
                rows_ref[at : at + PACK, column * LANES : (column + 1) * LANES] = got_ref[
                    source, unit : unit + PACK
                ]
    copies = []
    first = 0
    for size in TAKEN:
        row = iota((size, LANES), 0) + first
        put = jnp.concatenate(
            [(places[tile : tile + 1] == row).astype(f32).astype(bf16) for tile in range(RUN // LANES)], axis=1
        )
        part = pl.ds(first, size)
        out_ref[part] = jnp.dot(put, rows_ref[...], preferred_element_type=f32).astype(bf16)
        copies.append(pltpu.make_async_copy(out_ref.at[part], out_hbm.at[part], sems.at[len(copies) + 1]))
        copies[-1].start()
        first += size
    for copy in copies:
        copy.wait()


def unpack(got):
    return pl.pallas_call(
        unpack_kernel,
        out_shape=jax.ShapeDtypeStruct((RUN, D), bf16),
        in_specs=[whole()],
        out_specs=whole(pl.ANY),
        scratch_shapes=[
            pltpu.VMEM((RUN, D), bf16),
            pltpu.VMEM((RUN, D), bf16),
            pltpu.VMEM((1, LANES), jnp.int32),
            pltpu.SMEM((1, LANES), jnp.int32),
            pltpu.SemaphoreType.DMA((1 + len(TAKEN),)),
        ],
        compiler_params=pltpu.CompilerParams(vmem_limit_bytes=40 * 2**20),
        name="unpack",
    )(got)


def local(tokens, norm_gain, norm_bias, qkv_weight, out_weight, segment_ids, dest_map):
    sent = front(tokens, norm_gain, norm_bias, qkv_weight, out_weight, segment_ids, dest_map)
    got = lax.all_to_all(sent, "seq", split_axis=0, concat_axis=0, tiled=True)
    return unpack(got)


def solution(mesh):
    placed = (P(("dp", "seq"), None), P(), P(), P(), P(), P(("dp", "seq")), P(("dp", "seq")))
    return jax.shard_map(
        local, mesh=mesh, in_specs=placed, out_specs=P(("dp", "seq"), None), check_vma=False
    )
```
